32 devices in a mesh: cand: 4 (over x, core), blk: 4 (over z), feat: 2 (over y).
Axes of the slice: x: 2, y: 2, z: 4, core: 2. Of those that a mesh axis runs over, the one named last changes fastest.
Arguments:
- embeddings: float32 [32768, 1024], P(('cand', 'blk'), 'feat'), may hold values from -12 to 12
- winners: int32 [32, 3], replicated, may hold values from 0 to 32767, as said below
Outputs:
- columns: float32 [32, 3, 32768], P(None, None, ('cand', 'blk'))
- gains: float32 [32, 32768], P(None, ('cand', 'blk'))
- best: float32 [32, 3], replicated
The draws below stay inside these ranges and needn't reach their ends.
Inputs may be any that keep to these rules, and one draw needn't show every extreme that they name: winners[b,k] lies in [k * 10922, (k + 1) * 10922), so the winners of a session are distinct.
All inputs are finite; a program needn't handle non-finite values.
Results may differ from the reference program's by a relative error of at most 0.00012.
Values sent between devices are 32-bit elements; how exact they have to be, the bound alone decides.
A program may use at most 64 MiB of HBM per device.

```python
import math
import jax
import jax.numpy as jnp
from jax import lax

D = 1024
SESSIONS = 32
STEPS = 3
CANDS = 32768


def pick_winners(key):
    third = CANDS // STEPS
    picks = jax.random.randint(key, (SESSIONS, STEPS), 0, third)
    offsets = jnp.arange(STEPS, dtype=jnp.int32) * third
    return (picks + offsets[None, :]).astype(jnp.int32)


def draw_winners(key, part):
    return pick_winners(jax.random.fold_in(key, 11))


def draw_embeddings(key, part):
    chosen = pick_winners(jax.random.fold_in(key, 11))
    key_rows = jax.random.fold_in(key, 21)
    key_scale = jax.random.fold_in(key, 22)
    drawn = jnp.clip(jax.random.normal(key_rows, (CANDS, D), jnp.float32), -6.0, 6.0)
    scale = jnp.exp(jax.random.uniform(key_scale, (CANDS,), jnp.float32, math.log(0.2), math.log(2.0)))
    sessions = jnp.arange(SESSIONS, dtype=jnp.int32)
    step_index = jnp.arange(STEPS, dtype=jnp.int32)
    low_step = 1 + sessions // 2 % (STEPS - 1)
    forced = (sessions[:, None] % 2 == 1) & (step_index[None, :] == low_step[:, None])
    winner_scale = jnp.where(forced, 0.2, 1.0).astype(jnp.float32)
    flat = chosen.reshape(SESSIONS * STEPS)
    scale = scale.at[flat].set(1.0)
    scale = scale.at[flat].min(winner_scale.reshape(SESSIONS * STEPS))
    return (drawn * scale[:, None]).astype(jnp.float32)


def setup_inputs(seed: int = 0) -> dict:
    keys = jax.random.split(jax.random.key(seed), 3)
    embeddings = draw_embeddings(jax.random.fold_in(keys[2], 71), 0)
    winners = draw_winners(jax.random.fold_in(keys[2], 71), 0)
    return {"embeddings": embeddings, "winners": winners}


def reference(embeddings, winners):
    gains0 = lax.optimization_barrier(jnp.sum(embeddings * embeddings, axis=1)) / D
    gains = jnp.broadcast_to(gains0[None, :], (SESSIONS, CANDS)).astype(jnp.float32)
    columns = jnp.zeros((SESSIONS, STEPS, CANDS), jnp.float32)
    best_list = []
    for k in range(STEPS):
        best_list.append(lax.optimization_barrier(jnp.max(gains, axis=1)))
        chosen = winners[:, k].astype(jnp.int32)
        rows = embeddings[chosen]
        inner = jnp.dot(rows, embeddings.T, precision=lax.Precision.HIGHEST, preferred_element_type=jnp.float32) / D
        c_at = jnp.take_along_axis(columns, chosen[:, None, None], axis=2)[:, :, 0]
        d_at = jnp.take_along_axis(gains, chosen[:, None], axis=1)[:, 0]
        carried = jnp.einsum('bs,bsn->bn', c_at, columns, precision=lax.Precision.HIGHEST)
        update = (inner - carried) / jnp.sqrt(jnp.maximum(d_at, 0.1))[:, None]
        columns = columns.at[:, k, :].set(update)
        gains = gains - update * update
    return (columns, gains, jnp.stack(best_list, axis=1))
```

```python
import functools
import jax
import jax.numpy as jnp
from jax import lax
from jax.experimental import pallas as pl
from jax.experimental.pallas import tpu as pltpu
from jax.sharding import PartitionSpec as P

MESH = pl.DeviceIdType.MESH
F32 = jnp.float32
LANES = 128
SUB = 8


def spans(rows_here, group, steps):
    third = rows_here * group // steps
    return [(k * third // rows_here, ((k + 1) * third - 1) // rows_here) for k in range(steps)]


def kernel(cfg, win_ref, emb_hbm, col_ref, gain_ref, best_ref,
           emb, picked, slots, rows, part, inpart, gram, ingram, sq, insq, top, intop,
           load_sem, rs_send, rs_recv, ag_send, ag_recv, sq_send, sq_recv,
           gr_send, gr_recv, in_send, in_recv, top_send, top_recv):
    group, blks, feats, sessions, steps, chunk, total_width = cfg
    rows_here, width = emb_hbm.shape
    me = lax.axis_index("cand") * blks + lax.axis_index("blk")
    myfeat = lax.axis_index("feat")
    lane_blocks = width // LANES
    pieces = (sessions // SUB) * lane_blocks
    offset = me * rows_here

    def peer(index):
        return {"cand": index // blks, "blk": lax.rem(index, blks)}

    def mate(d):
        return {"feat": lax.rem(myfeat + d, feats)}

    def owner(index):
        return index < pieces

    load = pltpu.make_async_copy(emb_hbm, emb, load_sem)
    load.start()
    barrier = pltpu.get_barrier_semaphore()
    for d in range(1, group):
        pl.semaphore_signal(barrier, inc=1, device_id=peer(lax.rem(me + d, group)), device_id_type=MESH)
    for d in range(1, feats):
        pl.semaphore_signal(barrier, inc=1, device_id=mate(d), device_id_type=MESH)
    load.wait()

    span = spans(rows_here, group, steps)
    for k in range(steps):
        for b in range(sessions):
            at = win_ref[b, k] - offset
            inside = jnp.logical_and(at >= 0, at < rows_here)
            safe = jnp.clip(at, 0, rows_here - 1)
            row = emb[pl.ds(safe, 1), :]
            picked[k, b : b + 1, :] = jnp.where(inside, row, jnp.zeros_like(row))
    pl.semaphore_wait(barrier, group - 1 + feats - 1)

    def tile_at(index):
        r = pl.multiple_of(index // lane_blocks * SUB, SUB)
        c = pl.multiple_of(lax.rem(index, lane_blocks) * LANES, LANES)
        return pl.ds(r, SUB), pl.ds(c, LANES)

    def scatter_copy(k, d):
        to = lax.rem(me + d, group)
        at = lax.rem(to, pieces)
        r, c = tile_at(at)
        return pltpu.make_async_remote_copy(
            src_ref=picked.at[k, r, c],
            dst_ref=slots.at[k, me - span[k][0]],
            send_sem=rs_send.at[k, d - 1],
            recv_sem=rs_recv.at[k, me - span[k][0]],
            device_id=peer(to),
            device_id_type=MESH,
        )

    def contributes(k):
        return jnp.logical_and(me >= span[k][0], me <= span[k][1])

    for k in range(steps):
        @pl.when(contributes(k))
        def _(k=k):
            for d in range(1, group):
                @pl.when(owner(lax.rem(me + d, group)))
                def _(d=d):
                    scatter_copy(k, d).start()

            @pl.when(owner(me))
            def _():
                r, c = tile_at(lax.rem(me, pieces))
                slots[k, me - span[k][0]] = picked[k, r, c]

    for s in range(0, rows_here, 512):
        folded = jnp.zeros((512, LANES), F32)
        for l in range(lane_blocks):
            x = emb[s : s + 512, l * LANES : (l + 1) * LANES]
            folded = folded + x * x
        sq[:, s : s + 512] = jnp.sum(folded.T, axis=0, keepdims=True)

    def sq_copy(d):
        return pltpu.make_async_remote_copy(
            src_ref=sq, dst_ref=insq.at[d - 1], send_sem=sq_send.at[d - 1], recv_sem=sq_recv.at[d - 1],
            device_id=mate(d), device_id_type=MESH)

    def gather_copy(d, sender):
        r, c = tile_at(lax.rem(sender, pieces))
        return pltpu.make_async_remote_copy(
            src_ref=rows.at[:, r, c], dst_ref=rows.at[:, r, c],
            send_sem=ag_send.at[d - 1], recv_sem=ag_recv.at[d - 1],
            device_id=peer(lax.rem(me + d, group)), device_id_type=MESH)

    @pl.when(owner(me))
    def _():
        r, c = tile_at(lax.rem(me, pieces))
        for k in range(steps):
            for who in range(span[k][0], span[k][1] + 1):
                @pl.when(me != who)
                def _(k=k, who=who):
                    slot = slots.at[k, who - span[k][0]]
                    pltpu.make_async_remote_copy(
                        src_ref=slot, dst_ref=slot,
                        send_sem=rs_send.at[k, 0], recv_sem=rs_recv.at[k, who - span[k][0]],
                        device_id=peer(who), device_id_type=MESH).wait_recv()
        for k in range(steps):
            acc = slots[k, 0]
            for s in range(1, span[k][1] - span[k][0] + 1):
                acc = acc + slots[k, s]
            rows[k, r, c] = acc
        for d in range(1, group):
            gather_copy(d, me).start()

    for d in range(1, feats):
        sq_copy(d).start()

    for d in range(1, group):
        sender = lax.rem(me + group - d, group)
        @pl.when(owner(sender))
        def _(d=d, sender=sender):
            gather_copy(d, sender).wait_recv()

    lane = lax.broadcasted_iota(jnp.int32, (sessions, LANES), 1)
    pairs = [(t, u) for t in range(steps) for u in range(t + 1)]
    packed = jnp.zeros((sessions, LANES), F32)
    for i, (t, u) in enumerate(pairs):
        value = jnp.sum(rows[t] * rows[u], axis=1, keepdims=True)
        packed = jnp.where(lane == i, value, packed)
    gram[...] = packed

    def gram_copy(d):
        return pltpu.make_async_remote_copy(
            src_ref=gram, dst_ref=ingram.at[d - 1], send_sem=gr_send.at[d - 1], recv_sem=gr_recv.at[d - 1],
            device_id=mate(d), device_id_type=MESH)

    def part_copy(n, d):
        where = pl.ds(n * chunk, chunk)
        return pltpu.make_async_remote_copy(
            src_ref=part.at[:, where], dst_ref=inpart.at[d - 1, :, where],
            send_sem=in_send.at[n, d - 1], recv_sem=in_recv.at[n, d - 1],
            device_id=mate(d), device_id_type=MESH)

    chunks = rows_here // chunk
    lhs = rows[...].reshape(steps * sessions, width)
    for n in range(chunks):
        part[:, n * chunk : (n + 1) * chunk] = lax.dot_general(
            lhs, emb[n * chunk : (n + 1) * chunk, :], (((1,), (1,)), ((), ())),
            precision=lax.Precision.HIGHEST, preferred_element_type=F32)
        if n == 0:
            for d in range(1, feats):
                gram_copy(d).start()
        for d in range(1, feats):
            part_copy(n, d).start()

    for d in range(1, feats):
        sq_copy(d).wait_recv()
        gram_copy(d).wait_recv()
    both = gram[...]
    norms = sq[...]
    for d in range(1, feats):
        both = both + ingram[d - 1]
        norms = norms + insq[d - 1]
    both = both / total_width
    norms = norms / total_width
    factor = {}
    radius = []
    for t in range(steps):
        at = {u: both[:, i : i + 1] for i, (v, u) in enumerate(pairs) if v == t}
        lowered = at[t]
        for u in range(t):
            value = at[u]
            for w in range(u):
                value = value - factor[u, w] * factor[t, w]
            value = value / radius[u]
            factor[t, u] = value
            lowered = lowered - value * value
        radius.append(jnp.sqrt(jnp.maximum(lowered, 0.1)))

    tops = [None] * steps
    for n in range(chunks):
        for d in range(1, feats):
            part_copy(n, d).wait_recv()
        where = slice(n * chunk, (n + 1) * chunk)
        gains = jnp.broadcast_to(norms[:, where], (sessions, chunk))
        finished = []
        for t in range(steps):
            folded = gains[:, :LANES]
            for l in range(1, chunk // LANES):
                folded = jnp.maximum(folded, gains[:, l * LANES : (l + 1) * LANES])
            tops[t] = folded if tops[t] is None else jnp.maximum(tops[t], folded)
            inner = part[t * sessions : (t + 1) * sessions, where]
            for d in range(1, feats):
                inner = inner + inpart[d - 1, t * sessions : (t + 1) * sessions, where]
            inner = inner / total_width
            carried = jnp.zeros_like(inner)
            for u in range(t):
                carried = carried + factor[t, u] * finished[u]
            column = (inner - carried) / radius[t]
            finished.append(column)
            col_ref[t, :, where] = column
            gains = gains - column * column
        gain_ref[:, where] = gains

    pad = -(steps * sessions) % LANES
    stacked = jnp.concatenate(tops + ([jnp.zeros((pad, LANES), F32)] if pad else []), axis=0)
    top[...] = jnp.max(stacked.T, axis=0, keepdims=True)

    def top_copy(d):
        return pltpu.make_async_remote_copy(
            src_ref=top, dst_ref=intop.at[d - 1], send_sem=top_send.at[d - 1], recv_sem=top_recv.at[d - 1],
            device_id=peer(lax.rem(me + d, group)), device_id_type=MESH)

    for d in range(1, group):
        top_copy(d).start()

    for k in range(steps):
        @pl.when(contributes(k))
        def _(k=k):
            for d in range(1, group):
                @pl.when(owner(lax.rem(me + d, group)))
                def _(d=d):
                    scatter_copy(k, d).wait_send()

    @pl.when(owner(me))
    def _():
        for d in range(1, group):
            gather_copy(d, me).wait_send()

    for d in range(1, feats):
        sq_copy(d).wait_send()
        gram_copy(d).wait_send()
        for n in range(chunks):
            part_copy(n, d).wait_send()

    for d in range(1, group):
        top_copy(d).wait_recv()
    best = top[...]
    for d in range(1, group):
        best = jnp.maximum(best, intop[d - 1])
    best_ref[...] = best
    for d in range(1, group):
        top_copy(d).wait_send()


def body(cands, blks, feats, embeddings, winners):
    rows_here, width = embeddings.shape
    sessions, steps = winners.shape
    group = cands * blks
    chunk = min(256, rows_here)
    chunks = rows_here // chunk
    wide = max(b - a + 1 for a, b in spans(rows_here, group, steps))
    lanes = -(-steps * sessions // LANES) * LANES
    dma = pltpu.SemaphoreType.DMA
    cfg = (group, blks, feats, sessions, steps, chunk, width * feats)
    vmem = pl.BlockSpec(memory_space=pltpu.VMEM)
    columns, gains, best = pl.pallas_call(
        functools.partial(kernel, cfg),
        out_shape=(
            jax.ShapeDtypeStruct((steps, sessions, rows_here), F32),
            jax.ShapeDtypeStruct((sessions, rows_here), F32),
            jax.ShapeDtypeStruct((1, lanes), F32),
        ),
        in_specs=[pl.BlockSpec(memory_space=pltpu.SMEM), pl.BlockSpec(memory_space=pl.ANY)],
        out_specs=(vmem, vmem, vmem),
        scratch_shapes=[
            pltpu.VMEM((rows_here, width), F32),
            pltpu.VMEM((steps, sessions, width), F32),
            pltpu.VMEM((steps, wide, SUB, LANES), F32),
            pltpu.VMEM((steps, sessions, width), F32),
            pltpu.VMEM((steps * sessions, rows_here), F32),
            pltpu.VMEM((feats - 1, steps * sessions, rows_here), F32),
            pltpu.VMEM((sessions, LANES), F32),
            pltpu.VMEM((feats - 1, sessions, LANES), F32),
            pltpu.VMEM((1, rows_here), F32),
            pltpu.VMEM((feats - 1, 1, rows_here), F32),
            pltpu.VMEM((1, lanes), F32),
            pltpu.VMEM((group - 1, 1, lanes), F32),
            dma,
            dma((steps, group - 1)),
            dma((steps, wide)),
            dma((group - 1,)),
            dma((group - 1,)),
            dma((feats - 1,)),
            dma((feats - 1,)),
            dma((feats - 1,)),
            dma((feats - 1,)),
            dma((chunks, feats - 1)),
            dma((chunks, feats - 1)),
            dma((group - 1,)),
            dma((group - 1,)),
        ],
        compiler_params=pltpu.CompilerParams(collective_id=0, has_side_effects=True),
    )(winners, embeddings)
    best = best[0, : steps * sessions].reshape(steps, sessions).T
    return columns.transpose(1, 0, 2), gains, best


def solution(mesh):
    shape = mesh.shape
    return jax.shard_map(
        functools.partial(body, shape["cand"], shape["blk"], shape["feat"]),
        mesh=mesh,
        in_specs=(P(("cand", "blk"), "feat"), P()),
        out_specs=(P(None, None, ("cand", "blk")), P(None, ("cand", "blk")), P()),
        check_vma=False,
    )
```

```python
import functools
import jax
import jax.numpy as jnp
from jax import lax
from jax.experimental import pallas as pl
from jax.experimental.pallas import tpu as pltpu
from jax.sharding import PartitionSpec as P

MESH = pl.DeviceIdType.MESH
F32 = jnp.float32
LANES = 128
SUB = 8


def spans(rows_here, group, steps):
    third = rows_here * group // steps
    return [(k * third // rows_here, ((k + 1) * third - 1) // rows_here) for k in range(steps)]


def kernel(cfg, win_hbm, emb_hbm, col_hbm, gain_hbm, best_ref,
           win_ref, col_ref, gain_ref, emb, picked, slots, rows, part, inpart, gram, ingram, sq, insq, top, intop,
           win_sem, load_sem, out_sem, rs_send, rs_recv, ag_send, ag_recv, sq_send, sq_recv,
           gr_send, gr_recv, in_send, in_recv, top_send, top_recv):
    group, blks, feats, sessions, steps, chunk, total_width = cfg
    rows_here, width = emb_hbm.shape
    me = lax.axis_index("cand") * blks + lax.axis_index("blk")
    myfeat = lax.axis_index("feat")
    lane_blocks = width // LANES
    pieces = (sessions // SUB) * lane_blocks
    offset = me * rows_here

    def peer(index):
        return {"cand": index // blks, "blk": lax.rem(index, blks)}

    def mate(d):
        return {"feat": lax.rem(myfeat + d, feats)}

    def owner(index):
        return index < pieces

    load = pltpu.make_async_copy(emb_hbm, emb, load_sem)
    load.start()
    win_load = pltpu.make_async_copy(win_hbm, win_ref, win_sem)
    win_load.start()
    barrier = pltpu.get_barrier_semaphore()
    for d in range(1, group):
        pl.semaphore_signal(barrier, inc=1, device_id=peer(lax.rem(me + d, group)), device_id_type=MESH)
    for d in range(1, feats):
        pl.semaphore_signal(barrier, inc=1, device_id=mate(d), device_id_type=MESH)
    win_load.wait()
    load.wait()

    span = spans(rows_here, group, steps)
    for k in range(steps):
        for b in range(sessions):
            at = win_ref[k, b] - offset
            inside = jnp.logical_and(at >= 0, at < rows_here)
            safe = jnp.clip(at, 0, rows_here - 1)
            row = emb[pl.ds(safe, 1), :]
            picked[k, b : b + 1, :] = jnp.where(inside, row, jnp.zeros_like(row))
    pl.semaphore_wait(barrier, group - 1 + feats - 1)

    def tile_at(index):
        r = pl.multiple_of(index // lane_blocks * SUB, SUB)
        c = pl.multiple_of(lax.rem(index, lane_blocks) * LANES, LANES)
        return pl.ds(r, SUB), pl.ds(c, LANES)

    def scatter_copy(k, d):
        to = lax.rem(me + d, group)
        at = lax.rem(to, pieces)
        r, c = tile_at(at)
        return pltpu.make_async_remote_copy(
            src_ref=picked.at[k, r, c],
            dst_ref=slots.at[k, me - span[k][0]],
            send_sem=rs_send.at[k, d - 1],
            recv_sem=rs_recv.at[k, me - span[k][0]],
            device_id=peer(to),
            device_id_type=MESH,
        )

    def contributes(k):
        return jnp.logical_and(me >= span[k][0], me <= span[k][1])

    for k in range(steps):
        @pl.when(contributes(k))
        def _(k=k):
            for d in range(1, group):
                @pl.when(owner(lax.rem(me + d, group)))
                def _(d=d):
                    scatter_copy(k, d).start()

            @pl.when(owner(me))
            def _():
                r, c = tile_at(lax.rem(me, pieces))
                slots[k, me - span[k][0]] = picked[k, r, c]

    def sq_copy(d):
        return pltpu.make_async_remote_copy(
            src_ref=sq, dst_ref=insq.at[d - 1], send_sem=sq_send.at[d - 1], recv_sem=sq_recv.at[d - 1],
            device_id=mate(d), device_id_type=MESH)

    def gather_copy(d, sender):
        r, c = tile_at(lax.rem(sender, pieces))
        return pltpu.make_async_remote_copy(
            src_ref=rows.at[:, r, c], dst_ref=rows.at[:, r, c],
            send_sem=ag_send.at[d - 1], recv_sem=ag_recv.at[d - 1],
            device_id=peer(lax.rem(me + d, group)), device_id_type=MESH)

    @pl.when(owner(me))
    def _():
        r, c = tile_at(lax.rem(me, pieces))
        for k in range(steps):
            for who in range(span[k][0], span[k][1] + 1):
                @pl.when(me != who)
                def _(k=k, who=who):
                    slot = slots.at[k, who - span[k][0]]
                    pltpu.make_async_remote_copy(
                        src_ref=slot, dst_ref=slot,
                        send_sem=rs_send.at[k, 0], recv_sem=rs_recv.at[k, who - span[k][0]],
                        device_id=peer(who), device_id_type=MESH).wait_recv()
        for k in range(steps):
            acc = slots[k, 0]
            for s in range(1, span[k][1] - span[k][0] + 1):
                acc = acc + slots[k, s]
            rows[k, r, c] = acc
        for d in range(1, group):
            gather_copy(d, me).start()

    for d in range(1, group):
        sender = lax.rem(me + group - d, group)
        @pl.when(owner(sender))
        def _(d=d, sender=sender):
            gather_copy(d, sender).wait_recv()

    lane = lax.broadcasted_iota(jnp.int32, (sessions, LANES), 1)
    pairs = [(t, u) for t in range(steps) for u in range(t + 1)]

    def gram_copy(d):
        return pltpu.make_async_remote_copy(
            src_ref=gram, dst_ref=ingram.at[d - 1], send_sem=gr_send.at[d - 1], recv_sem=gr_recv.at[d - 1],
            device_id=mate(d), device_id_type=MESH)

    def part_copy(n, d):
        return pltpu.make_async_remote_copy(
            src_ref=part.at[n], dst_ref=inpart.at[d - 1, n],
            send_sem=in_send.at[n, d - 1], recv_sem=in_recv.at[n, d - 1],
            device_id=mate(d), device_id_type=MESH)

    chunks = rows_here // chunk
    lhs = rows[...].reshape(steps * sessions, width)
    for n in range(chunks):
        part[n] = lax.dot_general(
            lhs, emb[n * chunk : (n + 1) * chunk, :], (((1,), (1,)), ((), ())),
            precision=lax.Precision.HIGHEST, preferred_element_type=F32)
        for d in range(1, feats):
            part_copy(n, d).start()
        if n == 0:
            packed = jnp.zeros((sessions, LANES), F32)
            for i, (t, u) in enumerate(pairs):
                value = jnp.sum(rows[t] * rows[u], axis=1, keepdims=True)
                packed = jnp.where(lane == i, value, packed)
            gram[...] = packed
            for d in range(1, feats):
                gram_copy(d).start()

    for s in range(0, rows_here, 512):
        folded = jnp.zeros((512, LANES), F32)
        for l in range(lane_blocks):
            x = emb[s : s + 512, l * LANES : (l + 1) * LANES]
            folded = folded + x * x
        sq[:, s : s + 512] = jnp.sum(folded.T, axis=0, keepdims=True)

    for d in range(1, feats):
        sq_copy(d).start()

    for d in range(1, feats):
        sq_copy(d).wait_recv()
        gram_copy(d).wait_recv()
    both = gram[...]
    norms = sq[...]
    for d in range(1, feats):
        both = both + ingram[d - 1]
        norms = norms + insq[d - 1]
    both = both / total_width
    norms = norms / total_width
    factor = {}
    radius = []
    for t in range(steps):
        at = {u: both[:, i : i + 1] for i, (v, u) in enumerate(pairs) if v == t}
        lowered = at[t]
        for u in range(t):
            value = at[u]
            for w in range(u):
                value = value - factor[u, w] * factor[t, w]
            value = value / radius[u]
            factor[t, u] = value
            lowered = lowered - value * value
        radius.append(jnp.sqrt(jnp.maximum(lowered, 0.1)))

    def out_copies(n):
        where = pl.ds(n * chunk, chunk)
        return (
            pltpu.make_async_copy(col_ref.at[:, :, where], col_hbm.at[:, :, where], out_sem.at[0, n]),
            pltpu.make_async_copy(gain_ref.at[:, where], gain_hbm.at[:, where], out_sem.at[1, n]),
        )

    tops = [None] * steps
    for n in range(chunks):
        for d in range(1, feats):
            part_copy(n, d).wait_recv()
        where = slice(n * chunk, (n + 1) * chunk)
        gains = jnp.broadcast_to(norms[:, where], (sessions, chunk))
        finished = []
        for t in range(steps):
            folded = gains[:, :LANES]
            for l in range(1, chunk // LANES):
                folded = jnp.maximum(folded, gains[:, l * LANES : (l + 1) * LANES])
            tops[t] = folded if tops[t] is None else jnp.maximum(tops[t], folded)
            inner = part[n, t * sessions : (t + 1) * sessions, :]
            for d in range(1, feats):
                inner = inner + inpart[d - 1, n, t * sessions : (t + 1) * sessions, :]
            inner = inner / total_width
            carried = jnp.zeros_like(inner)
            for u in range(t):
                carried = carried + factor[t, u] * finished[u]
            column = (inner - carried) / radius[t]
            finished.append(column)
            col_ref[t, :, where] = column
            gains = gains - column * column
        gain_ref[:, where] = gains
        for copy in out_copies(n):
            copy.start()

    pad = -(steps * sessions) % LANES
    stacked = jnp.concatenate(tops + ([jnp.zeros((pad, LANES), F32)] if pad else []), axis=0)
    top[...] = jnp.max(stacked.T, axis=0, keepdims=True)

    def top_copy(d):
        return pltpu.make_async_remote_copy(
            src_ref=top, dst_ref=intop.at[d - 1], send_sem=top_send.at[d - 1], recv_sem=top_recv.at[d - 1],
            device_id=peer(lax.rem(me + d, group)), device_id_type=MESH)

    for d in range(1, group):
        top_copy(d).start()

    for n in range(chunks):
        for copy in out_copies(n):
            copy.wait()

    for k in range(steps):
        @pl.when(contributes(k))
        def _(k=k):
            for d in range(1, group):
                @pl.when(owner(lax.rem(me + d, group)))
                def _(d=d):
                    scatter_copy(k, d).wait_send()

    @pl.when(owner(me))
    def _():
        for d in range(1, group):
            gather_copy(d, me).wait_send()

    for d in range(1, feats):
        sq_copy(d).wait_send()
        gram_copy(d).wait_send()
        for n in range(chunks):
            part_copy(n, d).wait_send()

    for d in range(1, group):
        top_copy(d).wait_recv()
    best = top[...]
    for d in range(1, group):
        best = jnp.maximum(best, intop[d - 1])
    best_ref[...] = best
    for d in range(1, group):
        top_copy(d).wait_send()


def deliver(col_in, gain_in, best_in, col_out, gain_out, best_out, col_sem, gain_sem):
    col_copy = pltpu.make_async_copy(col_in, col_out, col_sem)
    gain_copy = pltpu.make_async_copy(gain_in, gain_out, gain_sem)
    col_copy.start()
    gain_copy.start()
    steps, sessions = best_out.shape
    for k in range(steps):
        best_out[k : k + 1, :] = best_in[:, k * sessions : (k + 1) * sessions]
    col_copy.wait()
    gain_copy.wait()


def body(cands, blks, feats, embeddings, winners):
    rows_here, width = embeddings.shape
    sessions, steps = winners.shape
    group = cands * blks
    chunk = min(256, rows_here)
    chunks = rows_here // chunk
    wide = max(b - a + 1 for a, b in spans(rows_here, group, steps))
    lanes = -(-steps * sessions // LANES) * LANES
    dma = pltpu.SemaphoreType.DMA
    cfg = (group, blks, feats, sessions, steps, chunk, width * feats)
    vmem = pl.BlockSpec(memory_space=pltpu.VMEM)
    hbm = pl.BlockSpec(memory_space=pl.ANY)
    columns, gains, best = pl.pallas_call(
        functools.partial(kernel, cfg),
        out_shape=(
            jax.ShapeDtypeStruct((steps, sessions, rows_here), F32),
            jax.ShapeDtypeStruct((sessions, rows_here), F32),
            jax.ShapeDtypeStruct((1, lanes), F32),
        ),
        in_specs=[pl.BlockSpec(memory_space=pltpu.HBM)] * 2,
        out_specs=(hbm, hbm, vmem),
        scratch_shapes=[
            pltpu.SMEM((steps, sessions), jnp.int32),
            pltpu.VMEM((steps, sessions, rows_here), F32),
            pltpu.VMEM((sessions, rows_here), F32),
            pltpu.VMEM((rows_here, width), F32),
            pltpu.VMEM((steps, sessions, width), F32),
            pltpu.VMEM((steps, wide, SUB, LANES), F32),
            pltpu.VMEM((steps, sessions, width), F32),
            pltpu.VMEM((chunks, steps * sessions, chunk), F32),
            pltpu.VMEM((feats - 1, chunks, steps * sessions, chunk), F32),
            pltpu.VMEM((sessions, LANES), F32),
            pltpu.VMEM((feats - 1, sessions, LANES), F32),
            pltpu.VMEM((1, rows_here), F32),
            pltpu.VMEM((feats - 1, 1, rows_here), F32),
            pltpu.VMEM((1, lanes), F32),
            pltpu.VMEM((group - 1, 1, lanes), F32),
            dma,
            dma,
            dma((2, chunks)),
            dma((steps, group - 1)),
            dma((steps, wide)),
            dma((group - 1,)),
            dma((group - 1,)),
            dma((feats - 1,)),
            dma((feats - 1,)),
            dma((feats - 1,)),
            dma((feats - 1,)),
            dma((chunks, feats - 1)),
            dma((chunks, feats - 1)),
            dma((group - 1,)),
            dma((group - 1,)),
        ],
        compiler_params=pltpu.CompilerParams(collective_id=0, has_side_effects=True, vmem_limit_bytes=50 * 2**20),
    )(winners.T, embeddings)
    columns, gains, best = pl.pallas_call(
        deliver,
        out_shape=(
            jax.ShapeDtypeStruct((steps, sessions, rows_here), F32),
            jax.ShapeDtypeStruct((sessions, rows_here), F32),
            jax.ShapeDtypeStruct((steps, sessions), F32),
        ),
        in_specs=[hbm, hbm, vmem],
        out_specs=(hbm, hbm, vmem),
        scratch_shapes=[dma, dma],
        compiler_params=pltpu.CompilerParams(vmem_limit_bytes=4 * 2**20),
    )(columns, gains, best)
    return columns.transpose(1, 0, 2), gains, best.T


def solution(mesh):
    shape = mesh.shape
    return jax.shard_map(
        functools.partial(body, shape["cand"], shape["blk"], shape["feat"]),
        mesh=mesh,
        in_specs=(P(("cand", "blk"), "feat"), P()),
        out_specs=(P(None, None, ("cand", "blk")), P(None, ("cand", "blk")), P()),
        check_vma=False,
    )
```
